32 devices in a mesh: dp: 4 (over y, z), cp: 8 (over x, core).
Axes of the slice: x: 4, y: 2, z: 2, core: 2. Of those that a mesh axis runs over, the one named last changes fastest.
The devices are a block of a 4x4x8 slice.
Arguments:
- vis_feat: bfloat16 [32, 4096, 1152], P(('dp', 'cp')), parts along dimension 0
- text_emb: bfloat16 [16384, 2048], P(('dp', 'cp')), parts along dimension 0
- img_pos: int32 [32], P('dp'), parts along dimension 0
- grad_y: bfloat16 [16384, 2048], P(('dp', 'cp')), parts along dimension 0
- pn_gain: bfloat16 [1152], replicated
- w_proj: bfloat16 [1152, 2048], replicated
- pre_gain: bfloat16 [2048], replicated
- w_query: bfloat16 [2048, 2048], replicated
- w_key: bfloat16 [2048, 256], replicated
- w_value: bfloat16 [2048, 256], replicated
- q_gain: bfloat16 [256], replicated
- k_gain: bfloat16 [256], replicated
- w_out: bfloat16 [2048, 2048], replicated
- post_gain: bfloat16 [2048], replicated
Outputs:
- output 1: bfloat16 [16384, 2048], P(('dp', 'cp')), parts along dimension 0
- output 2: bfloat16 [16384, 2048], P(('dp', 'cp')), parts along dimension 0
- output 3: bfloat16 [32, 4096, 1152], P(('dp', 'cp')), parts along dimension 0
- output 4: bfloat16 [4608], P('dp'), parts along dimension 0
- output 5: bfloat16 [4608, 2048], P('dp'), parts along dimension 0
- output 6: bfloat16 [8192], P('dp'), parts along dimension 0
- output 7: bfloat16 [8192, 2048], P('dp'), parts along dimension 0
- output 8: bfloat16 [8192, 256], P('dp'), parts along dimension 0
- output 9: bfloat16 [8192, 256], P('dp'), parts along dimension 0
- output 10: bfloat16 [1024], P('dp'), parts along dimension 0
- output 11: bfloat16 [1024], P('dp'), parts along dimension 0
- output 12: bfloat16 [8192, 2048], P('dp'), parts along dimension 0
- output 13: bfloat16 [8192], P('dp'), parts along dimension 0
There are 4 independent parts. The reference program is written for one: setup_inputs(seed, part) draws one part's arguments, and reference() takes and returns one part's arrays. A program takes and returns all parts, laid end to end along the dimension named above; an argument that names none is the same for every part.
All inputs are finite; a program needn't handle non-finite values.
Results may differ from the reference program's by a relative error of at most 0.02.
Values are sent between devices in bfloat16 or wider.
A program may use at most 768 MiB of HBM per device.

```python
import functools
import jax
import jax.numpy as jnp
from jax import lax

D = 2048
HEADS = 8
KV_HEADS = 1
HEAD = 256
DV = 1152
SEQ_DEV = 512
IMG_DEV = 1
GROUP = 8
GRID = 64
POOL = 4
SEQ = SEQ_DEV * GROUP
N_IMG = IMG_DEV * GROUP
SIDE = GRID // POOL
BLOCK = SIDE * SIDE
EPS = 1e-6
ROPE_BASE = 1000000.0
ROPE_SCALE = 8.0
NEG_BIG = -1e30


def place_images(rng_key):
    gap_key, perm_key = jax.random.split(rng_key)
    first_start = SEQ_DEV - BLOCK // 2
    spare = SEQ - N_IMG * BLOCK - first_start
    raw_gap = jax.random.randint(gap_key, (N_IMG,), 0, 8)
    weight = raw_gap * raw_gap * raw_gap
    gap_total = jnp.maximum(jnp.sum(weight), 1)
    gap_rows = spare * weight // gap_total
    slot_start = first_start + jnp.arange(N_IMG) * BLOCK + jnp.cumsum(gap_rows) - gap_rows
    slot_order = jax.random.permutation(perm_key, N_IMG)
    return slot_start[slot_order].astype(jnp.int32)


def draw_normal(rng_key, arr_shape, std_scale):
    return (jax.random.normal(rng_key, arr_shape, jnp.float32) * std_scale).astype(jnp.bfloat16)


def setup_inputs(seed: int = 0, part: int = 0) -> dict:
    base_key = jax.random.key(seed)
    part_keys = jax.random.split(jax.random.fold_in(base_key, part), 4)
    weight_keys = jax.random.split(jax.random.key(seed + 1), 10)
    return {
        'vis_feat': draw_normal(part_keys[0], (N_IMG, GRID * GRID, DV), 1.0),
        'text_emb': draw_normal(part_keys[1], (SEQ, D), 1.0),
        'img_pos': place_images(part_keys[2]),
        'grad_y': draw_normal(part_keys[3], (SEQ, D), 1.0),
        'pn_gain': draw_normal(weight_keys[0], (DV,), 0.3),
        'w_proj': draw_normal(weight_keys[1], (DV, D), DV ** -0.5),
        'pre_gain': draw_normal(weight_keys[2], (D,), 0.3),
        'w_query': draw_normal(weight_keys[3], (D, HEADS * HEAD), D ** -0.5),
        'w_key': draw_normal(weight_keys[4], (D, KV_HEADS * HEAD), D ** -0.5),
        'w_value': draw_normal(weight_keys[5], (D, KV_HEADS * HEAD), D ** -0.5),
        'q_gain': draw_normal(weight_keys[6], (HEAD,), 0.3),
        'k_gain': draw_normal(weight_keys[7], (HEAD,), 0.3),
        'w_out': draw_normal(weight_keys[8], (HEADS * HEAD, D), (HEADS * HEAD) ** -0.5),
        'post_gain': draw_normal(weight_keys[9], (D,), 0.3),
    }


def rms_scale(values, gain_vec):
    wide_vals = values.astype(jnp.float32)
    mean_sq = jnp.mean(wide_vals * wide_vals, axis=-1, keepdims=True)
    return wide_vals * lax.rsqrt(mean_sq + EPS) * (1.0 + gain_vec.astype(jnp.float32))


def rope_tables(positions):
    inv_freq = ROPE_BASE ** (-jnp.arange(0, HEAD, 2).astype(jnp.float32) / HEAD)
    rot_angle = (positions.astype(jnp.float32) / ROPE_SCALE)[:, None] * inv_freq[None, :]
    rot_angle = jnp.concatenate([rot_angle, rot_angle], axis=-1)
    return jnp.cos(rot_angle)[:, None, :], jnp.sin(rot_angle)[:, None, :]


def apply_rope(values, cos_t, sin_t):
    half_dim = values.shape[-1] // 2
    rotated = jnp.concatenate([-values[..., half_dim:], values[..., :half_dim]], axis=-1)
    return values * cos_t + rotated * sin_t


def project(vis_feat, pn_gain, w_proj):
    img_count = vis_feat.shape[0]
    patch_grid = vis_feat.reshape(img_count, SIDE, POOL, SIDE, POOL, DV).astype(jnp.float32)
    pooled = (jnp.sum(patch_grid, axis=(2, 4)) / (POOL * POOL)).astype(jnp.bfloat16)
    normed = rms_scale(pooled.reshape(img_count * BLOCK, DV), pn_gain).astype(jnp.bfloat16)
    return jnp.dot(normed, w_proj, preferred_element_type=jnp.float32).astype(jnp.bfloat16)


def attend_block(q_blk, start_blk, blk_index, k_heads, v_heads):
    groups = HEADS // KV_HEADS
    q_pos = blk_index * SEQ_DEV + jnp.arange(SEQ_DEV)
    key_pos = jnp.arange(SEQ)
    in_image = (start_blk[:, None] >= 0) & (key_pos[None, :] >= start_blk[:, None]) & (key_pos[None, :] < start_blk[:, None] + BLOCK)
    visible = (key_pos[None, :] <= q_pos[:, None]) | in_image
    q_grp = q_blk.reshape(SEQ_DEV, KV_HEADS, groups, HEAD).astype(jnp.float32)
    scores = jnp.einsum('qkgd,skd->kgqs', q_grp, k_heads.astype(jnp.float32)) * HEAD ** -0.5
    scores = jnp.where(visible[None, None], scores, NEG_BIG)
    prob_lo = jax.nn.softmax(scores, axis=-1).astype(jnp.bfloat16)
    attn_blk = jnp.einsum('kgqs,skd->qkgd', prob_lo.astype(jnp.float32), v_heads.astype(jnp.float32))
    return attn_blk.astype(jnp.bfloat16).reshape(SEQ_DEV, HEADS * HEAD)


def forward(vis_feat, text_emb, pn_gain, w_proj, pre_gain, w_query, w_key, w_value, q_gain, k_gain, w_out, post_gain, img_pos):
    soft_tok = project(vis_feat, pn_gain, w_proj)
    img_rows = (img_pos[:, None] + jnp.arange(BLOCK)[None, :]).reshape(-1)
    merged = text_emb.at[img_rows].set(soft_tok)
    starts = jnp.full((SEQ,), -1, jnp.int32).at[img_rows].set(jnp.repeat(img_pos, BLOCK))
    hidden = rms_scale(merged, pre_gain).astype(jnp.bfloat16)
    q_raw = jnp.dot(hidden, w_query, preferred_element_type=jnp.float32).astype(jnp.bfloat16).reshape(SEQ, HEADS, HEAD)
    k_raw = jnp.dot(hidden, w_key, preferred_element_type=jnp.float32).astype(jnp.bfloat16).reshape(SEQ, KV_HEADS, HEAD)
    v_heads = jnp.dot(hidden, w_value, preferred_element_type=jnp.float32).astype(jnp.bfloat16).reshape(SEQ, KV_HEADS, HEAD)
    cos_t, sin_t = rope_tables(jnp.arange(SEQ))
    q_heads = apply_rope(rms_scale(q_raw, q_gain), cos_t, sin_t).astype(jnp.bfloat16)
    k_heads = apply_rope(rms_scale(k_raw, k_gain), cos_t, sin_t).astype(jnp.bfloat16)
    block_fn = jax.checkpoint(attend_block)
    attn_out = lax.map(lambda blk_args: block_fn(blk_args[0], blk_args[1], blk_args[2], k_heads, v_heads), (q_heads.reshape(GROUP, SEQ_DEV, HEADS, HEAD), starts.reshape(GROUP, SEQ_DEV), jnp.arange(GROUP)))
    attn_out = attn_out.reshape(SEQ, HEADS * HEAD)
    proj_out = jnp.dot(attn_out, w_out, preferred_element_type=jnp.float32).astype(jnp.bfloat16)
    return (merged.astype(jnp.float32) + rms_scale(proj_out, post_gain)).astype(jnp.bfloat16)


def reference(vis_feat, text_emb, img_pos, grad_y, pn_gain, w_proj, pre_gain, w_query, w_key, w_value, q_gain, k_gain, w_out, post_gain):
    y_out, pullback = jax.vjp(functools.partial(forward, img_pos=img_pos), vis_feat, text_emb, pn_gain, w_proj, pre_gain, w_query, w_key, w_value, q_gain, k_gain, w_out, post_gain)
    grad_list = pullback(grad_y)
    return (y_out, grad_list[1], grad_list[0], grad_list[2], grad_list[3], grad_list[4], grad_list[5], grad_list[6], grad_list[7], grad_list[8], grad_list[9], grad_list[10], grad_list[11])
```

```python
import functools
import jax
import jax.numpy as jnp
from jax import lax
from jax.experimental import pallas as pl
from jax.experimental.pallas import tpu as pltpu
from jax.sharding import PartitionSpec as P

GRID = 64
POOL = 4
EPS = 1e-6
ROPE_BASE = 1000000.0
ROPE_SCALE = 8.0
NEG_BIG = -1e30
STRIPS = 4
ROWS = 256
F32 = jnp.float32
BF16 = jnp.bfloat16
ONE_BUF = pl.Buffered(1)


def dot_nn(lhs, rhs):
    return lax.dot_general(lhs, rhs, (((1,), (0,)), ((), ())), preferred_element_type=F32)


def dot_nt(lhs, rhs):
    return lax.dot_general(lhs, rhs, (((1,), (1,)), ((), ())), preferred_element_type=F32)


def inv_rms(wide):
    return lax.rsqrt(jnp.mean(wide * wide, axis=-1, keepdims=True) + EPS)


def norm_back(d_out, wide, inv, gain1):
    d_scaled = d_out * gain1
    unit = wide * inv
    d_in = inv * (d_scaled - unit * jnp.mean(d_scaled * unit, axis=-1, keepdims=True))
    d_gain = jnp.sum(d_out * unit, axis=0, keepdims=True)
    return d_in, d_gain


def resident(shape, col=None):
    if col is None:
        return pl.BlockSpec(shape, lambda *_: (0,) * len(shape), pipeline_mode=ONE_BUF)
    return pl.BlockSpec(shape, lambda *_: (0, col), pipeline_mode=ONE_BUF)


def pool_matrix(out_rows, in_rows, transpose):
    side = GRID // POOL
    shape = (in_rows, out_rows) if transpose else (out_rows, in_rows)
    out_id = lax.broadcasted_iota(jnp.int32, shape, 1 if transpose else 0)
    in_id = lax.broadcasted_iota(jnp.int32, shape, 0 if transpose else 1)
    target = (in_id // (GRID * POOL)) * side + (in_id % GRID) // POOL
    return jnp.where(out_id == target, 1.0, 0.0).astype(BF16)


def pool_kernel(vis_ref, gain_ref, pooled_ref, normed_ref):
    weights = pool_matrix(pooled_ref.shape[0], vis_ref.shape[0], False)
    pooled = (dot_nn(weights, vis_ref[...]) * (1.0 / (POOL * POOL))).astype(BF16)
    pooled_ref[...] = pooled
    wide = pooled.astype(F32)
    normed_ref[...] = (wide * inv_rms(wide) * (1.0 + gain_ref[...])).astype(BF16)


def pool_and_norm(vis_rows, gain):
    rows, dim = vis_rows.shape
    step_in = STRIPS * GRID * POOL
    step_out = step_in // (POOL * POOL)
    out = jax.ShapeDtypeStruct((rows // (POOL * POOL), dim), BF16)
    out_spec = pl.BlockSpec((step_out, dim), lambda i: (i, 0))
    return pl.pallas_call(
        pool_kernel, grid=(rows // step_in,),
        in_specs=[pl.BlockSpec((step_in, dim), lambda i: (i, 0)), resident((1, dim))],
        out_specs=[out_spec, out_spec], out_shape=[out, out],
        cost_estimate=pl.CostEstimate(flops=2 * rows * dim * step_out, bytes_accessed=rows * dim * 2, transcendentals=0),
        name='pool')(vis_rows, gain)


def unpool_kernel(d_ref, pooled_ref, gain_ref, out_ref, g_ref):
    wide = pooled_ref[...].astype(F32)
    d_pooled, d_gain = norm_back(d_ref[...].astype(F32), wide, inv_rms(wide), 1.0 + gain_ref[...])

    @pl.when(pl.program_id(0) == 0)
    def _():
        g_ref[...] = jnp.zeros_like(g_ref)

    g_ref[...] += d_gain
    spread = (d_pooled.astype(BF16).astype(F32) * (1.0 / (POOL * POOL))).astype(BF16)
    out_ref[...] = dot_nn(pool_matrix(spread.shape[0], out_ref.shape[0], True), spread).astype(BF16)


def unpool(d_normed, pooled, gain):
    rows, dim = pooled.shape
    step_out = STRIPS * GRID * POOL
    step_in = step_out // (POOL * POOL)
    in_spec = pl.BlockSpec((step_in, dim), lambda i: (i, 0))
    return pl.pallas_call(
        unpool_kernel, grid=(rows // step_in,),
        in_specs=[in_spec, in_spec, resident((1, dim))],
        out_specs=[pl.BlockSpec((step_out, dim), lambda i: (i, 0)), pl.BlockSpec((1, dim), lambda i: (0, 0))],
        out_shape=[jax.ShapeDtypeStruct((rows * POOL * POOL, dim), BF16), jax.ShapeDtypeStruct((1, dim), F32)],
        cost_estimate=pl.CostEstimate(flops=32 * rows * dim * step_in, bytes_accessed=32 * rows * dim, transcendentals=0),
        name='unpool')(d_normed, pooled, gain)


def rotate(unit, cos, sin):
    half = cos.shape[-1]
    first, second = unit[:, :half], unit[:, half:]
    return jnp.concatenate([first * cos - second * sin, second * cos + first * sin], axis=-1)


def rotate_back(d_out, cos, sin):
    half = cos.shape[-1]
    first, second = d_out[:, :half], d_out[:, half:]
    return jnp.concatenate([first * cos + second * sin, second * cos - first * sin], axis=-1)


def front_kernel(row_ref, text_ref, all_ref, wp_ref, pre_ref, wk_ref, wv_ref, kg_ref, cos_ref, sin_ref,
                 rows_ref, merged_ref, hidden_ref, kraw_ref, kv_ref):
    row_id = row_ref[...]
    cols = lax.broadcasted_iota(jnp.int32, (row_id.shape[0], all_ref.shape[0]), 1)
    pick = jnp.where(cols == row_id, 1.0, 0.0).astype(BF16)
    normed_rows = dot_nn(pick, all_ref[...]).astype(BF16)
    rows_ref[...] = normed_rows
    soft = dot_nn(normed_rows, wp_ref[...]).astype(BF16)
    wide = jnp.where(row_id >= 0, soft.astype(F32), text_ref[...].astype(F32))
    merged_ref[...] = wide.astype(BF16)
    hidden = (wide * inv_rms(wide) * (1.0 + pre_ref[...])).astype(BF16)
    hidden_ref[...] = hidden
    k_raw = dot_nn(hidden, wk_ref[...]).astype(BF16)
    kraw_ref[...] = k_raw
    k_wide = k_raw.astype(F32)
    unit = k_wide * inv_rms(k_wide) * (1.0 + kg_ref[...])
    head = k_raw.shape[1]
    kv_ref[:, :head] = rotate(unit, cos_ref[...], sin_ref[...]).astype(BF16)
    kv_ref[:, head:] = dot_nn(hidden, wv_ref[...]).astype(BF16)


def front(row_id, text, normed_all, w_proj, pre_gain, w_key, w_value, k_gain, cos, sin):
    seq, dim = text.shape
    n_img, dim_v = normed_all.shape
    head = w_key.shape[1]

    def by_row(width):
        return pl.BlockSpec((ROWS, width), lambda i: (i, 0))

    flops = 2 * seq * (n_img * dim_v + dim_v * dim + 2 * dim * head)
    return pl.pallas_call(
        front_kernel, grid=(seq // ROWS,),
        in_specs=[by_row(1), by_row(dim), resident(normed_all.shape), resident(w_proj.shape), resident((1, dim)),
                  resident(w_key.shape), resident(w_value.shape), resident((1, head)), by_row(cos.shape[1]), by_row(cos.shape[1])],
        out_specs=[by_row(dim_v), by_row(dim), by_row(dim), by_row(head), by_row(2 * head)],
        out_shape=[jax.ShapeDtypeStruct((seq, w), BF16) for w in (dim_v, dim, dim, head, 2 * head)],
        cost_estimate=pl.CostEstimate(flops=flops, bytes_accessed=flops // 200, transcendentals=0),
        name='front')(row_id, text, normed_all, w_proj, pre_gain, w_key, w_value, k_gain, cos, sin)


def query_kernel(hid_ref, wq_ref, qg_ref, cos_ref, sin_ref, qraw_ref, qs_ref):
    q_raw = dot_nn(hid_ref[...], wq_ref[...]).astype(BF16)
    qraw_ref[...] = q_raw
    wide = q_raw.astype(F32)
    unit = wide * inv_rms(wide) * (1.0 + qg_ref[...])
    q_head = rotate(unit, cos_ref[...], sin_ref[...]).astype(BF16)
    qs_ref[...] = (q_head.astype(F32) * q_head.shape[1] ** -0.5).astype(BF16)


def query(hidden, w_query, q_gain, cos, sin):
    seq, dim = hidden.shape
    head = q_gain.shape[1]
    heads = w_query.shape[1] // head
    out = jax.ShapeDtypeStruct((seq, heads * head), BF16)
    by_head = pl.BlockSpec((seq, head), lambda h: (0, h))
    return pl.pallas_call(
        query_kernel, grid=(heads,),
        in_specs=[resident(hidden.shape), pl.BlockSpec((dim, head), lambda h: (0, h)), resident((1, head)),
                  resident(cos.shape), resident(sin.shape)],
        out_specs=[by_head, by_head], out_shape=[out, out],
        cost_estimate=pl.CostEstimate(flops=2 * seq * dim * heads * head, bytes_accessed=dim * heads * head * 2, transcendentals=0),
        name='query')(hidden, w_query, q_gain, cos, sin)


def visible_mask(key_base, q_base, start, shape, block_len):
    key_pos = key_base + lax.broadcasted_iota(jnp.int32, shape, 0)
    q_pos = q_base + lax.broadcasted_iota(jnp.int32, shape, 1)
    return (key_pos <= q_pos) | ((key_pos >= start) & (key_pos < start + block_len))


def key_rows(index, width):
    return pl.ds(pl.multiple_of(index * width, width), width)


def attn_kernel(block_len, pair, rank_ref, qs_ref, k_ref, v_ref, start_ref, o_ref, lse_ref, vt_ref, acc_ref, m_ref, l_ref):
    seq = qs_ref.shape[0]
    head = k_ref.shape[1]
    total = k_ref.shape[0]
    rank = rank_ref[0]
    start = start_ref[...]

    @pl.when(pl.program_id(0) == 0)
    def _():
        @pl.loop(0, total // seq)
        def _(i):
            vt_ref[:, key_rows(i, seq)] = v_ref[key_rows(i, seq), :].astype(F32).T.astype(BF16)

    def block(base, width, masked, first):
        rows = pl.ds(pl.multiple_of(base, width), width)
        k_blk = k_ref[rows, :]
        vt_blk = vt_ref[:, rows]
        if masked:
            mask = visible_mask(base, rank * seq, start, (width, seq), block_len)
        scores = [dot_nt(k_blk, qs_ref[:, j * head:(j + 1) * head]) for j in range(pair)]
        for j in range(pair):
            score = jnp.where(mask, scores[j], NEG_BIG) if masked else scores[j]
            top = jnp.max(score, axis=0, keepdims=True)
            if first:
                m_new = top
                prob = jnp.exp(score - m_new)
                l_ref[j] = jnp.sum(prob, axis=0, keepdims=True)
                acc_ref[j] = dot_nn(vt_blk, prob.astype(BF16))
            else:
                m_old = m_ref[j]
                m_new = jnp.maximum(m_old, top)
                alpha = jnp.exp(m_old - m_new)
                prob = jnp.exp(score - m_new)
                l_ref[j] = l_ref[j] * alpha + jnp.sum(prob, axis=0, keepdims=True)
                acc_ref[j] = acc_ref[j] * alpha + dot_nn(vt_blk, prob.astype(BF16))
            m_ref[j] = m_new

    block(rank * seq, seq, True, True)

    @pl.when(rank * seq + seq < total)
    def _():
        block((rank + 1) * seq, block_len, True, False)

    @pl.loop(0, rank)
    def _(i):
        block(i * seq, seq, False, False)

    for j in range(pair):
        denom = l_ref[j]
        o_ref[:, j * head:(j + 1) * head] = (acc_ref[j] / denom).T.astype(BF16)
        lse_ref[j] = m_ref[j] + jnp.log(denom)


def attention(rank, qs, kv_all, blk_start, head, block_len):
    seq, width = qs.shape
    heads = width // head
    pair = 2 if heads % 2 == 0 else 1
    total = kv_all.shape[0]
    flops = 4 * seq * heads * head * total
    by_head = pl.BlockSpec((seq, pair * head), lambda h, *_: (0, h))
    grid_spec = pltpu.PrefetchScalarGridSpec(
        num_scalar_prefetch=1, grid=(heads // pair,),
        in_specs=[by_head, resident((total, head), 0), resident((total, head), 1), resident((1, seq))],
        out_specs=[by_head, pl.BlockSpec((pair, 1, seq), lambda h, *_: (h, 0, 0))],
        scratch_shapes=[pltpu.VMEM((head, total), BF16), pltpu.VMEM((pair, head, seq), F32),
                        pltpu.VMEM((pair, 1, seq), F32), pltpu.VMEM((pair, 1, seq), F32)])
    return pl.pallas_call(
        functools.partial(attn_kernel, block_len, pair), grid_spec=grid_spec,
        out_shape=[jax.ShapeDtypeStruct((seq, width), BF16), jax.ShapeDtypeStruct((heads, 1, seq), F32)],
        cost_estimate=pl.CostEstimate(flops=flops, bytes_accessed=flops // 1000, transcendentals=0),
        name='attention')(rank, qs, kv_all, kv_all, blk_start)


def post_kernel(o_ref, merged_ref, dy_ref, wo_ref, gain_ref, y_ref, dproj_ref, dattn_ref, g_ref):
    proj = dot_nn(o_ref[...], wo_ref[...]).astype(BF16).astype(F32)
    inv = inv_rms(proj)
    gain1 = 1.0 + gain_ref[...]
    y_ref[...] = (merged_ref[...].astype(F32) + proj * inv * gain1).astype(BF16)
    d_in, d_gain = norm_back(dy_ref[...].astype(F32), proj, inv, gain1)

    @pl.when(pl.program_id(0) == 0)
    def _():
        g_ref[...] = jnp.zeros_like(g_ref)

    g_ref[...] += d_gain
    d_proj = d_in.astype(BF16)
    dproj_ref[...] = d_proj
    dattn_ref[...] = dot_nt(d_proj, wo_ref[...]).astype(BF16)


def post(attn_out, merged, grad_y, w_out, gain):
    seq, dim = merged.shape
    width = attn_out.shape[1]

    def by_row(cols):
        return pl.BlockSpec((ROWS, cols), lambda i: (i, 0))

    flops = 4 * seq * dim * width
    return pl.pallas_call(
        post_kernel, grid=(seq // ROWS,),
        in_specs=[by_row(width), by_row(dim), by_row(dim), resident(w_out.shape), resident((1, dim))],
        out_specs=[by_row(dim), by_row(dim), by_row(width), pl.BlockSpec((1, dim), lambda i: (0, 0))],
        out_shape=[jax.ShapeDtypeStruct((seq, dim), BF16), jax.ShapeDtypeStruct((seq, dim), BF16),
                   jax.ShapeDtypeStruct((seq, width), BF16), jax.ShapeDtypeStruct((1, dim), F32)],
        cost_estimate=pl.CostEstimate(flops=flops, bytes_accessed=flops // 200, transcendentals=0),
        name='post')(attn_out, merged, grad_y, w_out, gain)


def back_kernel(block_len, pair, rank_ref, qs_ref, do_ref, o_ref, k_ref, v_ref, start_ref, lse_ref, qraw_ref, cos_ref, sin_ref, gain_ref,
                dq_ref, g_ref, dkv_ref, kt_ref, acc_ref):
    seq = qs_ref.shape[0]
    head = k_ref.shape[1]
    total = k_ref.shape[0]
    rank = rank_ref[0]
    start = start_ref[...]

    @pl.when(pl.program_id(0) == 0)
    def _():
        g_ref[...] = jnp.zeros_like(g_ref)

        @pl.loop(0, total // seq)
        def _(i):
            kt_ref[:, key_rows(i, seq)] = k_ref[key_rows(i, seq), :].astype(F32).T.astype(BF16)
            dkv_ref[key_rows(i, seq), :] = jnp.zeros((seq, 2 * head), F32)

    cols = [slice(j * head, (j + 1) * head) for j in range(pair)]
    deltas = []
    for j in range(pair):
        both = do_ref[:, cols[j]].astype(F32) * o_ref[:, cols[j]].astype(F32)
        delta = jnp.sum(both, axis=1, keepdims=True)
        deltas.append(jnp.broadcast_to(delta, (seq, 128)).T[0:1, :])
    acc_ref[...] = jnp.zeros_like(acc_ref)

    def block(base, width, masked):
        rows = pl.ds(pl.multiple_of(base, width), width)
        k_blk = k_ref[rows, :]
        v_blk = v_ref[rows, :]
        kt_blk = kt_ref[:, rows]
        if masked:
            mask = visible_mask(base, rank * seq, start, (width, seq), block_len)
        d_k = None
        d_v = None
        for j in range(pair):
            qs = qs_ref[:, cols[j]]
            d_o = do_ref[:, cols[j]]
            score = dot_nt(k_blk, qs)
            if masked:
                score = jnp.where(mask, score, NEG_BIG)
            prob = jnp.exp(score - lse_ref[j])
            d_score = (prob * (dot_nt(v_blk, d_o) - deltas[j])).astype(BF16)
            v_part = dot_nn(prob.astype(BF16), d_o)
            k_part = dot_nn(d_score, qs)
            d_v = v_part if d_v is None else d_v + v_part
            d_k = k_part if d_k is None else d_k + k_part
            acc_ref[j] += dot_nn(kt_blk, d_score)
        dkv_ref[rows, :head] += d_k
        dkv_ref[rows, head:] += d_v

    block(rank * seq, seq, True)

    @pl.when(rank * seq + seq < total)
    def _():
        block((rank + 1) * seq, block_len, True)

    @pl.loop(0, rank)
    def _(i):
        block(i * seq, seq, False)

    gain1 = 1.0 + gain_ref[...]
    for j in range(pair):
        d_q = (acc_ref[j] * head ** -0.5).T.astype(BF16).astype(F32)
        d_unit = rotate_back(d_q, cos_ref[...], sin_ref[...])
        wide = qraw_ref[:, cols[j]].astype(F32)
        d_raw, d_gain = norm_back(d_unit, wide, inv_rms(wide), gain1)
        dq_ref[:, cols[j]] = d_raw.astype(BF16)
        g_ref[...] += d_gain


def attention_back(rank, qs, d_attn, attn_out, kv_all, blk_start, lse, q_raw, cos, sin, q_gain, block_len):
    seq, width = qs.shape
    head = q_gain.shape[1]
    heads = width // head
    pair = 2 if heads % 2 == 0 else 1
    total = kv_all.shape[0]
    flops = 10 * seq * heads * head * total
    by_head = pl.BlockSpec((seq, pair * head), lambda h, *_: (0, h))
    grid_spec = pltpu.PrefetchScalarGridSpec(
        num_scalar_prefetch=1, grid=(heads // pair,),
        in_specs=[by_head, by_head, by_head, resident((total, head), 0), resident((total, head), 1), resident((1, seq)),
                  pl.BlockSpec((pair, 1, seq), lambda h, *_: (h, 0, 0)), by_head, resident(cos.shape), resident(sin.shape), resident((1, head))],
        out_specs=[by_head, pl.BlockSpec((1, head), lambda h, *_: (0, 0)), resident((total, 2 * head))],
        scratch_shapes=[pltpu.VMEM((head, total), BF16), pltpu.VMEM((pair, head, seq), F32)])
    return pl.pallas_call(
        functools.partial(back_kernel, block_len, pair), grid_spec=grid_spec,
        out_shape=[jax.ShapeDtypeStruct((seq, width), BF16), jax.ShapeDtypeStruct((1, head), F32),
                   jax.ShapeDtypeStruct((total, 2 * head), F32)],
        cost_estimate=pl.CostEstimate(flops=flops, bytes_accessed=flops // 1000, transcendentals=0),
        name='attention_back')(rank, qs, d_attn, attn_out, kv_all, kv_all, blk_start, lse, q_raw, cos, sin, q_gain)


def merge_layout(img_pos, dev_rank, seq_loc, block_len):
    q_pos = dev_rank * seq_loc + jnp.arange(seq_loc)
    offset = q_pos[:, None] - img_pos[None, :]
    in_blk = (offset >= 0) & (offset < block_len)
    is_img = jnp.any(in_blk, axis=1)
    flat_row = jnp.sum(jnp.where(in_blk, jnp.arange(img_pos.shape[0])[None, :] * block_len + offset, 0), axis=1)
    blk_start = jnp.where(is_img, q_pos - jnp.sum(jnp.where(in_blk, offset, 0), axis=1), -block_len)
    return q_pos, is_img, jnp.where(is_img, flat_row, -1), blk_start


def rope_tables(positions, head_dim):
    inv_freq = ROPE_BASE ** (-jnp.arange(0, head_dim, 2).astype(F32) / head_dim)
    angle = (positions.astype(F32) / ROPE_SCALE)[:, None] * inv_freq[None, :]
    return jnp.cos(angle), jnp.sin(angle)


def scatter_sum(partial):
    return lax.psum_scatter(partial, 'cp', scatter_dimension=0, tiled=True)


def solution(mesh):
    seq_spec = P(('dp', 'cp'))
    part_spec = P('dp')
    rep_spec = P()

    def device_body(vis_loc, text_loc, img_pos, grad_y, pn_gain, w_proj, pre_gain, w_query, w_key, w_value, q_gain, k_gain, w_out, post_gain):
        rank = lax.axis_index('cp')
        seq = text_loc.shape[0]
        dim_v = vis_loc.shape[2]
        head = q_gain.shape[0]
        block_len = (GRID // POOL) ** 2
        pn_row, pre_row, q_row, k_row, post_row = (g.astype(F32)[None, :] for g in (pn_gain, pre_gain, q_gain, k_gain, post_gain))
        q_pos, is_img, flat_row, blk_start = merge_layout(img_pos, rank, seq, block_len)
        cos, sin = rope_tables(q_pos, head)
        rank_arr = rank.astype(jnp.int32)[None]
        start_row = blk_start.astype(jnp.int32)[None, :]
        img_mask = is_img[:, None]

        pooled, normed = pool_and_norm(vis_loc.reshape(-1, dim_v), pn_row)
        normed_all = lax.all_gather(normed, 'cp', tiled=True)
        normed_rows, merged, hidden, k_raw, kv_loc = front(
            flat_row.astype(jnp.int32)[:, None], text_loc, normed_all, w_proj, pre_row, w_key, w_value, k_row, cos, sin)
        kv_all = lax.all_gather(kv_loc, 'cp', tiled=True)
        q_raw, qs = query(hidden, w_query, q_row, cos, sin)
        attn_out, lse = attention(rank_arr, qs, kv_all, start_row, head, block_len)
        y_loc, d_proj, d_attn, g_post = post(attn_out, merged, grad_y, w_out, post_row)
        g_out = scatter_sum(jnp.einsum('sh,sd->hd', attn_out, d_proj, preferred_element_type=F32))
        d_q, g_q_gain, dkv_part = attention_back(
            rank_arr, qs, d_attn, attn_out, kv_all, start_row, lse, q_raw, cos, sin, q_row, block_len)
        dkv = scatter_sum(dkv_part)
        g_query = scatter_sum(jnp.einsum('sd,sh->dh', hidden, d_q, preferred_element_type=F32))

        d_k = dkv[:, :head].astype(BF16).astype(F32)
        d_v = dkv[:, head:].astype(BF16)
        k_wide = k_raw.astype(F32)
        d_k_raw, g_k_gain = norm_back(rotate_back(d_k, cos, sin), k_wide, inv_rms(k_wide), 1.0 + k_row)
        d_kv = jnp.concatenate([d_k_raw.astype(BF16), d_v], axis=1)
        w_kv = jnp.concatenate([w_key, w_value], axis=1)
        d_hidden = jnp.einsum('sh,dh->sd', d_q, w_query, preferred_element_type=F32)
        d_hidden = (d_hidden + jnp.einsum('sh,dh->sd', d_kv, w_kv, preferred_element_type=F32)).astype(BF16)
        m_wide = merged.astype(F32)
        d_norm, g_pre = norm_back(d_hidden.astype(F32), m_wide, inv_rms(m_wide), 1.0 + pre_row)
        d_merged = (grad_y.astype(F32) + d_norm.astype(BF16).astype(F32)).astype(BF16)
        grad_text = jnp.where(img_mask, 0.0, d_merged).astype(BF16)
        d_soft = jnp.where(img_mask, d_merged, 0.0).astype(BF16)
        d_normed_rows = jnp.einsum('nd,cd->nc', d_soft, w_proj, preferred_element_type=F32).astype(BF16)
        pick = (flat_row[:, None] == jnp.arange(normed_all.shape[0])[None, :]).astype(BF16)
        d_normed_all = jnp.einsum('sn,sc->nc', pick, d_normed_rows, preferred_element_type=F32).astype(BF16)
        d_normed = scatter_sum(d_normed_all)
        g_kv = jnp.einsum('sd,sh->dh', hidden, d_kv, preferred_element_type=F32)
        g_proj_t = jnp.einsum('nd,nc->dc', d_soft, normed_rows, preferred_element_type=F32)
        g_mix = scatter_sum(jnp.concatenate([g_kv, g_proj_t], axis=1))
        grad_vis, g_pn = unpool(d_normed, pooled, pn_row)

        small = [g_pn[0], g_pre[0], g_q_gain[0], g_k_gain[0], g_post[0]]
        small_sum = lax.psum(jnp.concatenate(small), 'cp').astype(BF16)
        cuts = [0]
        for part in small:
            cuts.append(cuts[-1] + part.shape[0])
        g_pn, g_pre, g_q_gain, g_k_gain, g_post = (small_sum[a:b] for a, b in zip(cuts[:-1], cuts[1:]))
        g_mix = lax.all_gather(g_mix.astype(BF16), 'cp', tiled=True)
        g_out = lax.all_gather(g_out.astype(BF16), 'cp', tiled=True)
        g_query = lax.all_gather(g_query.astype(BF16), 'cp', tiled=True)
        g_key, g_value, g_proj = g_mix[:, :head], g_mix[:, head:2 * head], g_mix[:, 2 * head:].T
        return (y_loc, grad_text, grad_vis.reshape(vis_loc.shape), g_pn, g_proj, g_pre, g_query, g_key, g_value, g_q_gain, g_k_gain, g_out, g_post)

    in_specs = (seq_spec, seq_spec, part_spec, seq_spec) + (rep_spec,) * 10
    out_specs = (seq_spec, seq_spec, seq_spec) + (part_spec,) * 10
    return jax.shard_map(device_body, mesh=mesh, in_specs=in_specs, out_specs=out_specs, check_vma=False)
```
